512 devices in a mesh: gx: 16 (over y, z_lo), gy: 32 (over x, z_hi, core).
Axes of the slice: x: 4, y: 8, z: 8 (z_hi: 4, z_lo: 2; z = z_hi * 2 + z_lo), core: 2. Of those that a mesh axis runs over, the one named last changes fastest.
Arguments:
- fields: bfloat16 [8, 256, 512, 192], P(None, 'gx', 'gy'), may hold values from -6 to 6
- gain_window: float32 [192], replicated, may hold values from 0.1 to 1.9
- mixer_fine: bfloat16 [192, 576], replicated, may hold values from -3 to 3
- output_fine: bfloat16 [192, 192], replicated, may hold values from -0.4375 to 0.4375
- gain_hidden: float32 [192], replicated, may hold values from 0.1 to 1.9
- expand: bfloat16 [192, 768], replicated, may hold values from -0.4375 to 0.4375
- contract: bfloat16 [768, 192], replicated, may hold values from -0.21875 to 0.21875
- gain_merge: float32 [768], replicated, may hold values from 0.1 to 1.9
- merge_weight: bfloat16 [768, 384], replicated, may hold values from -0.21875 to 0.21875
- gain_coarse: float32 [384], replicated, may hold values from 0.1 to 1.9
- mixer_coarse: bfloat16 [384, 1152], replicated, may hold values from -2.1 to 2.1
- output_coarse: bfloat16 [384, 384], replicated, may hold values from -0.3125 to 0.3125
Outputs:
- merged: bfloat16 [8, 128, 256, 384], P(None, 'gx', 'gy')
- coarse: bfloat16 [8, 128, 256, 384], P(None, 'gx', 'gy')
The draws below stay inside these ranges and needn't reach their ends.
All inputs are finite; a program needn't handle non-finite values.
Results may differ from the reference program's by a relative error of at most 0.019.
Values may be sent and summed in bfloat16 or wider, within the bound.
No kernel may reach another device: no remote copies, remote signals or barrier semaphores. Data moves between devices by JAX's collectives and lax.ppermute only.
A program may use at most 128 MiB of HBM per device.

```python
import math
import jax
import jax.numpy as jnp
from jax import lax

BATCH = 8
WIN = 16
C2 = 192
C3 = 384
HID2 = 768
HEADS2 = 6
HEADS3 = 12
H2 = 256
W2 = 512
H3 = 128
W3 = 256


def normal_block(key, rows_count, columns):
    return jax.random.truncated_normal(key, -5.0, 5.0, (rows_count, columns), jnp.float32) / math.sqrt(rows_count)


def draw_fields(key, part):
    key_base = jax.random.fold_in(key, 0)
    values = jax.random.truncated_normal(key_base, -6.0, 6.0, (BATCH, H2, W2, C2), jnp.float32)
    return values.astype(jnp.bfloat16)


def draw_mixer_fine(key, part):
    key_base = jax.random.fold_in(key, 0)
    base = normal_block(key_base, C2, 3 * C2)
    values = base
    return jnp.clip(values, -3.0, 3.0).astype(jnp.bfloat16)


def draw_mixer_coarse(key, part):
    key_base = jax.random.fold_in(jax.random.fold_in(key, 7), 0)
    base = normal_block(key_base, C3, 3 * C3)
    values = base
    return jnp.clip(values, -2.1, 2.1).astype(jnp.bfloat16)


def scatter_about(rng, shape, scale, bound, kind=jnp.bfloat16):
    return jnp.clip(scale * jax.random.normal(rng, shape, jnp.float32), -bound, bound).astype(kind)


def setup_inputs(seed: int = 0) -> dict:
    key_of = jax.random.split(jax.random.key(seed), 13)
    return {
        "fields": draw_fields(jax.random.fold_in(key_of[12], 71), 0),
        "gain_window": jnp.clip(1.0 + 0.18 * jax.random.normal(key_of[1], (C2,), jnp.float32), 0.1, 1.9),
        "mixer_fine": draw_mixer_fine(jax.random.fold_in(key_of[12], 71), 0),
        "output_fine": scatter_about(key_of[3], (C2, C2), C2 ** -0.5, 0.4375),
        "gain_hidden": jnp.clip(1.0 + 0.18 * jax.random.normal(key_of[4], (C2,), jnp.float32), 0.1, 1.9),
        "expand": scatter_about(key_of[5], (C2, HID2), C2 ** -0.5, 0.4375),
        "contract": scatter_about(key_of[6], (HID2, C2), HID2 ** -0.5, 0.21875),
        "gain_merge": jnp.clip(1.0 + 0.18 * jax.random.normal(key_of[7], (4 * C2,), jnp.float32), 0.1, 1.9),
        "merge_weight": scatter_about(key_of[8], (4 * C2, C3), (4 * C2) ** -0.5, 0.21875),
        "gain_coarse": jnp.clip(1.0 + 0.18 * jax.random.normal(key_of[9], (C3,), jnp.float32), 0.1, 1.9),
        "mixer_coarse": draw_mixer_coarse(jax.random.fold_in(key_of[12], 71), 0),
        "output_coarse": scatter_about(key_of[11], (C3, C3), C3 ** -0.5, 0.3125),
    }


epsilon = 1e-05

def normalize(values, scaling):
    values = values.astype(jnp.float32)
    center = values - lax.optimization_barrier(jnp.mean(values, -1, keepdims=True))
    spread = lax.optimization_barrier(jnp.mean(center * center, -1, keepdims=True))
    return center * lax.rsqrt(spread + epsilon) * scaling.astype(jnp.float32)

def attend(query_rows, key_rows, value_rows, head_count):
    windows, length, channels = query_rows.shape
    head_size = channels // head_count
    split_query = query_rows.astype(jnp.float32).reshape(windows, length, head_count, head_size)
    split_keys = key_rows.astype(jnp.float32).reshape(windows, -1, head_count, head_size)
    split_values = value_rows.astype(jnp.float32).reshape(windows, -1, head_count, head_size)
    scores = jnp.einsum('nqhd,nkhd->nhqk', split_query, split_keys) / math.sqrt(head_size)
    highest = lax.optimization_barrier(jnp.max(scores, -1, keepdims=True))
    powers = jnp.exp(scores - highest)
    attention = (powers / lax.optimization_barrier(jnp.sum(powers, -1, keepdims=True))).astype(jnp.bfloat16)
    context = jnp.einsum('nhqk,nkhd->nqhd', attention.astype(jnp.float32), split_values)
    return context.reshape(windows, length, channels).astype(jnp.bfloat16)

def attention_layer(tokens, scaling, mixer, output_weight, head_count):
    channels = tokens.shape[-1]
    normed = normalize(tokens, scaling).astype(jnp.bfloat16)
    projected = jnp.dot(normed, mixer, preferred_element_type=jnp.float32).astype(jnp.bfloat16)
    context = attend(projected[..., :channels], projected[..., channels:2 * channels], projected[..., 2 * channels:], head_count)
    update = jnp.dot(context, output_weight, preferred_element_type=jnp.float32)
    return (tokens.astype(jnp.float32) + update).astype(jnp.bfloat16)

def feed_forward(tokens, scaling, expand, contract):
    normed = normalize(tokens, scaling).astype(jnp.bfloat16)
    hidden = jax.nn.gelu(jnp.dot(normed, expand, preferred_element_type=jnp.float32), approximate=False).astype(jnp.bfloat16)
    return (tokens.astype(jnp.float32) + jnp.dot(hidden, contract, preferred_element_type=jnp.float32)).astype(jnp.bfloat16)

def merge_patches(tokens, scaling, merge_weight):
    samples, height, breadth, channels = tokens.shape
    patches = tokens.reshape(samples, height // 2, 2, breadth // 2, 2, channels).transpose(0, 1, 3, 4, 2, 5)
    patches = patches.reshape(samples, height // 2, breadth // 2, 4 * channels)
    normed = normalize(patches, scaling).astype(jnp.bfloat16)
    return jnp.dot(normed, merge_weight, preferred_element_type=jnp.float32).astype(jnp.bfloat16)

def to_windows(tokens, window):
    samples, height, breadth, channels = tokens.shape
    blocks = tokens.reshape(samples, height // window, window, breadth // window, window, channels)
    return blocks.transpose(0, 1, 3, 2, 4, 5).reshape(samples * (height // window), breadth // window, window * window, channels)

def from_windows(blocks, samples, height, breadth, window):
    channels = blocks.shape[-1]
    tokens = blocks.reshape(samples, height // window, breadth // window, window, window, channels)
    return tokens.transpose(0, 1, 3, 2, 4, 5).reshape(samples, height, breadth, channels)

def reference(fields, gain_window, mixer_fine, output_fine, gain_hidden, expand, contract, gain_merge, merge_weight, gain_coarse, mixer_coarse, output_coarse):
    offset = WIN // 2
    rolled = jnp.roll(fields, (-offset, -offset), axis=(1, 2))

    def fine_block(blocks):
        attended = attention_layer(blocks, gain_window, mixer_fine, output_fine, HEADS2)
        return feed_forward(attended, gain_hidden, expand, contract)
    refined = lax.map(fine_block, to_windows(rolled, WIN))
    refined = jnp.roll(from_windows(refined, BATCH, H2, W2, WIN), (offset, offset), axis=(1, 2))
    merged = lax.map(lambda sample: merge_patches(sample[None], gain_merge, merge_weight)[0], refined)

    def coarse_block(blocks):
        return attention_layer(blocks, gain_coarse, mixer_coarse, output_coarse, HEADS3)
    coarse = from_windows(lax.map(coarse_block, to_windows(merged, WIN)), BATCH, H3, W3, WIN)
    return (merged, coarse)
```

```python
import functools
import math

import jax
import jax.numpy as jnp
from jax import lax
from jax.experimental import pallas as pl
from jax.experimental.pallas import tpu as pltpu
from jax.sharding import PartitionSpec as P

HEAD = 32
EPS = 1e-05
SCALE = math.log2(math.e) / math.sqrt(HEAD)
F32 = jnp.float32
BF16 = jnp.bfloat16


def dot(a, b):
    return jnp.dot(a, b, preferred_element_type=F32)


def dot_nt(a, b):
    return lax.dot_general(a, b, (((1,), (1,)), ((), ())), preferred_element_type=F32)


def iota(shape, dim):
    return lax.broadcasted_iota(jnp.int32, shape, dim)


def one_hot(rows, source):
    return jnp.where(iota((rows, rows), 1) == source, 1.0, 0.0).astype(BF16)


def normalize(values, scaling):
    center = values - jnp.mean(values, -1, keepdims=True)
    spread = jnp.mean(center * center, -1, keepdims=True)
    return center * lax.rsqrt(spread + EPS) * scaling


def pack_body(odd_ref, x_ref, own_ref, col_ref, row_ref, diag_ref, order_ref):
    @pl.when(pl.program_id(0) == 0)
    def _():
        odd = odd_ref[0]
        place = iota((256, 256), 0)
        piece = place // 64
        phase = (place // 16) % 4
        i = 2 * ((place // 4) % 4) + phase % 2
        j = 2 * (place % 4) + phase // 2
        bottom = jnp.where(piece < 2, 1, 0)
        keep = jnp.where((piece == 0) | (piece == 3), odd, 1 - odd)
        order_ref[...] = one_hot(256, (8 * bottom + i) * 16 + 8 * keep + j)

    samples = x_ref.shape[0]
    for n in range(samples):
        tokens = x_ref[n].reshape(256, 192)
        sorted_tokens = dot(order_ref[...], tokens)
        own_ref[n] = sorted_tokens[:64].astype(BF16)
        for slot, ref in enumerate((col_ref, row_ref, diag_ref)):
            part = sorted_tokens[64 * (slot + 1) : 64 * (slot + 2)]
            ref[n, :64, :] = part[:, :128].astype(BF16)
            ref[n, 64:, :] = jnp.concatenate([part[:32, 128:], part[32:, 128:]], 1).astype(BF16)


def pack(odd, fields):
    samples = fields.shape[0]
    step = 2
    piece = jax.ShapeDtypeStruct((samples, 96, 128), BF16)
    piece_spec = pl.BlockSpec((step, 96, 128), lambda n: (n, 0, 0))
    return pl.pallas_call(
        pack_body,
        grid=(samples // step,),
        in_specs=[
            pl.BlockSpec(memory_space=pltpu.SMEM),
            pl.BlockSpec((step, 16, 16, 192), lambda n: (n, 0, 0, 0)),
        ],
        out_specs=[pl.BlockSpec((step, 64, 192), lambda n: (n, 0, 0))] + [piece_spec] * 3,
        out_shape=[jax.ShapeDtypeStruct((samples, 64, 192), BF16)] + [piece] * 3,
        scratch_shapes=[pltpu.VMEM((256, 256), BF16)],
        name="pack",
    )(odd, fields)


def unpack(ref, n):
    low = ref[n, :64, :].astype(F32)
    high = ref[n, 64:, :].astype(F32)
    turned = pltpu.roll(high, 64, 1)
    return jnp.concatenate([low, jnp.concatenate([high, turned], 0)[:, :64]], 1)


def head_mask(head, last):
    lane = iota((1, 128), 1) // HEAD
    return jnp.where(jnp.minimum(lane, last) == head, 1.0, 0.0).astype(BF16)


def attend_group(queries, keys, values, heads):
    rows = queries.shape[0]
    length = keys.shape[0]
    powers = []
    weights = []
    for head in range(heads):
        mask = head_mask(head, heads - 1)
        scores = dot_nt(queries * mask, keys)
        highest = jnp.max(scores, -1, keepdims=True) * SCALE
        powers.append(jnp.exp2(scores * SCALE - highest).astype(BF16))
        weights.append(
            jnp.concatenate([values * mask, jnp.broadcast_to(mask, (length, 128))], 1)
        )
    sums = dot(jnp.concatenate(powers, 1), jnp.concatenate(weights, 0))
    return (sums[:, :128] / sums[:, 128:]).astype(BF16)


def gelu(x):
    return 0.5 * x * (1.0 + lax.erf(x * math.sqrt(0.5)))


def fine_body(
    own_ref,
    col_ref,
    row_ref,
    diag_ref,
    gain_window,
    mixer,
    output,
    gain_hidden,
    expand,
    contract,
    gain_merge,
    merge_weight,
    own_out,
    col_out,
    row_out,
    diag_out,
):
    for n in range(own_ref.shape[0]):
        tokens = jnp.concatenate(
            [own_ref[n].astype(F32), unpack(col_ref, n), unpack(row_ref, n), unpack(diag_ref, n)], 0
        )
        normed = normalize(tokens, gain_window[...]).astype(BF16)
        mixed = dot(normed, mixer[...]).astype(BF16)
        context = jnp.concatenate(
            [
                attend_group(mixed[:, :128], mixed[:, 256:384], mixed[:, 512:640], 4),
                attend_group(mixed[:, 128:256], mixed[:, 384:512], mixed[:, 640:], 2),
            ],
            1,
        )
        attended = (tokens + dot(context, output[...])).astype(BF16).astype(F32)
        normed = normalize(attended, gain_hidden[...]).astype(BF16)
        hidden = gelu(dot(normed, expand[...])).astype(BF16)
        refined = (attended + dot(hidden, contract[...])).astype(BF16).astype(F32)
        phases = [
            jnp.concatenate(
                [refined[64 * piece + 16 * k : 64 * piece + 16 * (k + 1)] for piece in range(4)], 0
            )
            for k in range(4)
        ]
        mean = sum(jnp.sum(part, -1, keepdims=True) for part in phases) / 768.0
        centers = [part - mean for part in phases]
        spread = sum(jnp.sum(part * part, -1, keepdims=True) for part in centers) / 768.0
        ratio = lax.rsqrt(spread + EPS)
        merged = sum(
            dot((centers[k] * ratio * gain_merge[k : k + 1, :]).astype(BF16), merge_weight[k])
            for k in range(4)
        ).astype(BF16)
        for slot, ref in enumerate((own_out, col_out, row_out, diag_out)):
            ref[n] = merged[16 * slot : 16 * (slot + 1)]


def whole(array):
    return pl.BlockSpec(array.shape, lambda n: (0,) * array.ndim)


def fine(own, col, row, diag, *weights):
    samples = own.shape[0]
    step = 1
    piece_spec = pl.BlockSpec((step, 96, 128), lambda n: (n, 0, 0))
    return pl.pallas_call(
        fine_body,
        grid=(samples // step,),
        in_specs=[pl.BlockSpec((step, 64, 192), lambda n: (n, 0, 0))]
        + [piece_spec] * 3
        + [whole(w) for w in weights],
        out_specs=[pl.BlockSpec((step, 16, 384), lambda n: (n, 0, 0))] * 4,
        out_shape=[jax.ShapeDtypeStruct((samples, 16, 384), BF16)] * 4,
        name="fine",
    )(own, col, row, diag, *weights)


def assemble_body(odd_ref, own_ref, col_ref, row_ref, diag_ref, out_ref):
    odd = odd_ref[0]
    place = iota((64, 64), 0)
    r = place // 8
    c = place % 8
    bottom = r // 4
    keep = jnp.where(c // 4 == odd, 1, 0)
    piece = jnp.where(bottom == 1, 1 - keep, 2 + keep)
    order = one_hot(64, piece * 16 + (r % 4) * 4 + c % 4)
    for n in range(own_ref.shape[0]):
        parts = jnp.concatenate([own_ref[n], col_ref[n], row_ref[n], diag_ref[n]], 0)
        out_ref[n] = dot(order, parts).astype(BF16)


def assemble(odd, *pieces):
    samples = pieces[0].shape[0]
    vmem = pl.BlockSpec(memory_space=pltpu.VMEM)
    return pl.pallas_call(
        assemble_body,
        in_specs=[pl.BlockSpec(memory_space=pltpu.SMEM)] + [vmem] * 4,
        out_specs=vmem,
        out_shape=jax.ShapeDtypeStruct((samples, 64, 384), BF16),
        name="assemble",
    )(odd, *pieces)


def coarse_body(mine_ref, a_ref, b_ref, c_ref, gain, mixer, output, out_ref):
    for n in range(mine_ref.shape[0]):
        mine = mine_ref[n].astype(F32)
        tokens = jnp.concatenate(
            [mine, a_ref[n].astype(F32), b_ref[n].astype(F32), c_ref[n].astype(F32)], 0
        )
        normed = normalize(tokens, gain[...]).astype(BF16)
        queries = dot(normed[:64], mixer[:, :384]).astype(BF16)
        pairs = dot(normed, mixer[:, 384:]).astype(BF16)
        context = jnp.concatenate(
            [
                attend_group(
                    queries[:, g * 128 : (g + 1) * 128],
                    pairs[:, g * 128 : (g + 1) * 128],
                    pairs[:, 384 + g * 128 : 384 + (g + 1) * 128],
                    4,
                )
                for g in range(3)
            ],
            1,
        )
        out_ref[n] = (mine + dot(context, output[...])).astype(BF16)


def coarse(tiles, *weights):
    samples = tiles[0].shape[0]
    step = 1
    spec = pl.BlockSpec((step, 64, 384), lambda n: (n, 0, 0))
    return pl.pallas_call(
        coarse_body,
        grid=(samples // step,),
        in_specs=[spec] * 4 + [whole(w) for w in weights],
        out_specs=spec,
        out_shape=jax.ShapeDtypeStruct((samples, 64, 384), BF16),
        name="coarse",
    )(*tiles, *weights)


def shards(
    rows,
    columns,
    fields,
    gain_window,
    mixer_fine,
    output_fine,
    gain_hidden,
    expand,
    contract,
    gain_merge,
    merge_weight,
    gain_coarse,
    mixer_coarse,
    output_coarse,
):
    samples = fields.shape[0]

    def moved(value, target, back=False):
        pairs = []
        for p in range(rows):
            for q in range(columns):
                to_p, to_q = target(p, q)
                pair = (p * columns + q, (to_p % rows) * columns + to_q % columns)
                pairs.append(pair[::-1] if back else pair)
        return lax.ppermute(value, ("gx", "gy"), pairs)

    def to_row(p, q):
        return p - 1, q

    def to_col(p, q):
        return p, q - 1 if p % 2 else q + 1

    def to_diag(p, q):
        return p - 1, q + 1 if p % 2 else q - 1

    odd = (lax.axis_index("gx") % 2).astype(jnp.int32).reshape(1)
    own, col, row, diag = pack(odd, fields)
    col = moved(col, to_col)
    row = moved(row, to_row)
    diag = moved(diag, to_diag)
    mixer = jnp.pad(mixer_fine.reshape(192, 3, 192), ((0, 0), (0, 0), (0, 64))).reshape(192, 768)
    own, col, row, diag = fine(
        own,
        col,
        row,
        diag,
        gain_window.reshape(1, 192),
        mixer,
        jnp.pad(output_fine, ((0, 64), (0, 0))),
        gain_hidden.reshape(1, 192),
        expand,
        contract,
        gain_merge.reshape(4, 192),
        merge_weight.reshape(4, 192, 384),
    )
    col = moved(col, to_col, True)
    row = moved(row, to_row, True)
    diag = moved(diag, to_diag, True)
    tile = assemble(odd, own, col, row, diag)
    beside = moved(tile, lambda p, q: (p ^ 1, q))
    twin = moved(tile, lambda p, q: (p, q ^ 1))
    beyond = moved(beside, lambda p, q: (p, q ^ 1))
    result = coarse(
        (tile, beside, twin, beyond), gain_coarse.reshape(1, 384), mixer_coarse, output_coarse
    )
    shape = (samples, 8, 8, 384)
    return tile.reshape(shape), result.reshape(shape)


def solution(mesh):
    place = P(None, "gx", "gy", None)
    body = functools.partial(shards, mesh.shape["gx"], mesh.shape["gy"])
    return jax.shard_map(
        body, mesh=mesh, in_specs=(place,) + (P(),) * 11, out_specs=(place, place), check_vma=False
    )
```

```python
import functools
import math

import jax
import jax.numpy as jnp
from jax import lax
from jax.experimental import pallas as pl
from jax.experimental.pallas import tpu as pltpu
from jax.sharding import PartitionSpec as P

HEAD = 32
EPS = 1e-05
SCALE = math.log2(math.e) / math.sqrt(HEAD)
F32 = jnp.float32
BF16 = jnp.bfloat16


def dot(a, b):
    return jnp.dot(a, b, preferred_element_type=F32)


def dot_nt(a, b):
    return lax.dot_general(a, b, (((1,), (1,)), ((), ())), preferred_element_type=F32)


def iota(shape, dim):
    return lax.broadcasted_iota(jnp.int32, shape, dim)


def one_hot(rows, source):
    return jnp.where(iota((rows, rows), 1) == source, 1.0, 0.0).astype(BF16)


def normalize(values, scaling):
    center = values - jnp.mean(values, -1, keepdims=True)
    spread = jnp.mean(center * center, -1, keepdims=True)
    return center * lax.rsqrt(spread + EPS) * scaling


def pack_body(odd_ref, x_ref, own_ref, col_ref, row_ref, diag_ref, order_ref):
    @pl.when(pl.program_id(0) == 0)
    def _():
        odd = odd_ref[0]
        place = iota((256, 256), 0)
        piece = place // 64
        phase = (place // 16) % 4
        i = 2 * ((place // 4) % 4) + phase % 2
        j = 2 * (place % 4) + phase // 2
        bottom = jnp.where(piece < 2, 1, 0)
        keep = jnp.where((piece == 0) | (piece == 3), odd, 1 - odd)
        order_ref[...] = one_hot(256, (8 * bottom + i) * 16 + 8 * keep + j)

    samples = x_ref.shape[0]
    for n in range(samples):
        tokens = x_ref[n].reshape(256, 192)
        sorted_tokens = dot(order_ref[...], tokens)
        own_ref[n] = sorted_tokens[:64].astype(BF16)
        for slot, ref in enumerate((col_ref, row_ref, diag_ref)):
            part = sorted_tokens[64 * (slot + 1) : 64 * (slot + 2)]
            ref[n, :64, :] = part[:, :128].astype(BF16)
            ref[n, 64:, :] = jnp.concatenate([part[:32, 128:], part[32:, 128:]], 1).astype(BF16)


def pack(odd, fields):
    samples = fields.shape[0]
    step = 2
    piece = jax.ShapeDtypeStruct((samples, 96, 128), BF16)
    piece_spec = pl.BlockSpec((step, 96, 128), lambda n: (n, 0, 0))
    return pl.pallas_call(
        pack_body,
        grid=(samples // step,),
        in_specs=[
            pl.BlockSpec(memory_space=pltpu.SMEM),
            pl.BlockSpec((step, 16, 16, 192), lambda n: (n, 0, 0, 0)),
        ],
        out_specs=[pl.BlockSpec((step, 64, 192), lambda n: (n, 0, 0))] + [piece_spec] * 3,
        out_shape=[jax.ShapeDtypeStruct((samples, 64, 192), BF16)] + [piece] * 3,
        scratch_shapes=[pltpu.VMEM((256, 256), BF16)],
        compiler_params=pltpu.CompilerParams(vmem_limit_bytes=16 << 20),
        name="pack",
    )(odd, fields)


def unpack(ref, n):
    low = ref[n, :64, :].astype(F32)
    high = ref[n, 64:, :].astype(F32)
    turned = pltpu.roll(high, 64, 1)
    return jnp.concatenate([low, jnp.concatenate([high, turned], 0)[:, :64]], 1)


def head_mask(head, last):
    lane = iota((1, 128), 1) // HEAD
    return jnp.where(jnp.minimum(lane, last) == head, 1.0, 0.0).astype(BF16)


def attend_group(queries, keys, values, heads):
    rows = queries.shape[0]
    length = keys.shape[0]
    masks = [head_mask(head, heads - 1) for head in range(heads)]
    scores = dot_nt(jnp.concatenate([queries * mask for mask in masks], 0), keys)
    highest = jnp.max(scores, -1, keepdims=True) * SCALE
    power = jnp.exp2(scores * SCALE - highest).astype(BF16)
    powers = [power[head * rows : (head + 1) * rows] for head in range(heads)]
    weights = [
        jnp.concatenate([values * mask, jnp.broadcast_to(mask, (length, 128))], 1) for mask in masks
    ]
    sums = dot(jnp.concatenate(powers, 1), jnp.concatenate(weights, 0))
    return (sums[:, :128] / sums[:, 128:]).astype(BF16)


def gelu(x):
    return 0.5 * x * (1.0 + lax.erf(x * math.sqrt(0.5)))


def fine_body(
    own_ref,
    col_ref,
    row_ref,
    diag_ref,
    gain_window,
    mixer,
    output,
    gain_hidden,
    expand,
    contract,
    gain_merge,
    merge_weight,
    own_out,
    col_out,
    row_out,
    diag_out,
):
    windows = own_ref.shape[0]
    tokens = jnp.concatenate(
        [
            part
            for n in range(windows)
            for part in (
                own_ref[n].astype(F32),
                unpack(col_ref, n),
                unpack(row_ref, n),
                unpack(diag_ref, n),
            )
        ],
        0,
    )
    normed = normalize(tokens, gain_window[...]).astype(BF16)
    mixed = dot(normed, mixer[...]).astype(BF16)
    contexts = []
    for n in range(windows):
        one = mixed[256 * n : 256 * (n + 1)]
        contexts.append(
            jnp.concatenate(
                [
                    attend_group(one[:, :128], one[:, 256:384], one[:, 512:640], 4),
                    attend_group(one[:, 128:256], one[:, 384:512], one[:, 640:], 2),
                ],
                1,
            )
        )
    context = jnp.concatenate(contexts, 0)
    attended = (tokens + dot(context, output[...])).astype(BF16).astype(F32)
    normed = normalize(attended, gain_hidden[...]).astype(BF16)
    hidden = gelu(dot(normed, expand[...])).astype(BF16)
    refined = (attended + dot(hidden, contract[...])).astype(BF16).astype(F32)
    phases = [
        jnp.concatenate(
            [
                refined[64 * piece + 16 * k : 64 * piece + 16 * (k + 1)]
                for piece in range(4 * windows)
            ],
            0,
        )
        for k in range(4)
    ]
    mean = sum(jnp.sum(part, -1, keepdims=True) for part in phases) / 768.0
    centers = [part - mean for part in phases]
    spread = sum(jnp.sum(part * part, -1, keepdims=True) for part in centers) / 768.0
    ratio = lax.rsqrt(spread + EPS)
    merged = sum(
        dot((centers[k] * ratio * gain_merge[k : k + 1, :]).astype(BF16), merge_weight[k])
        for k in range(4)
    ).astype(BF16)
    for n in range(windows):
        for slot, ref in enumerate((own_out, col_out, row_out, diag_out)):
            ref[n] = merged[64 * n + 16 * slot : 64 * n + 16 * (slot + 1)]


def whole(array):
    return pl.BlockSpec(array.shape, lambda n: (0,) * array.ndim)


def fine(own, col, row, diag, *weights):
    samples = own.shape[0]
    step = 4
    piece_spec = pl.BlockSpec((step, 96, 128), lambda n: (n, 0, 0))
    return pl.pallas_call(
        fine_body,
        grid=(samples // step,),
        in_specs=[pl.BlockSpec((step, 64, 192), lambda n: (n, 0, 0))]
        + [piece_spec] * 3
        + [whole(w) for w in weights],
        out_specs=[pl.BlockSpec((step, 16, 384), lambda n: (n, 0, 0))] * 4,
        out_shape=[jax.ShapeDtypeStruct((samples, 16, 384), BF16)] * 4,
        compiler_params=pltpu.CompilerParams(vmem_limit_bytes=32 << 20),
        name="fine",
    )(own, col, row, diag, *weights)


def assemble_body(odd_ref, own_ref, col_ref, row_ref, diag_ref, out_ref):
    odd = odd_ref[0]
    place = iota((64, 64), 0)
    r = place // 8
    c = place % 8
    bottom = r // 4
    keep = jnp.where(c // 4 == odd, 1, 0)
    piece = jnp.where(bottom == 1, 1 - keep, 2 + keep)
    order = one_hot(64, piece * 16 + (r % 4) * 4 + c % 4)
    for n in range(own_ref.shape[0]):
        parts = jnp.concatenate([own_ref[n], col_ref[n], row_ref[n], diag_ref[n]], 0)
        out_ref[n] = dot(order, parts).astype(BF16)


def assemble(odd, *pieces):
    samples = pieces[0].shape[0]
    vmem = pl.BlockSpec(memory_space=pltpu.VMEM)
    return pl.pallas_call(
        assemble_body,
        in_specs=[pl.BlockSpec(memory_space=pltpu.SMEM)] + [vmem] * 4,
        out_specs=vmem,
        out_shape=jax.ShapeDtypeStruct((samples, 64, 384), BF16),
        compiler_params=pltpu.CompilerParams(vmem_limit_bytes=8 << 20),
        name="assemble",
    )(odd, *pieces)


def coarse_body(mine_ref, a_ref, b_ref, c_ref, gain, mixer, output, out_ref):
    windows = mine_ref.shape[0]
    refs = (mine_ref, a_ref, b_ref, c_ref)
    tokens = jnp.concatenate([ref[n].astype(F32) for n in range(windows) for ref in refs], 0)
    mine = jnp.concatenate([tokens[256 * n : 256 * n + 64] for n in range(windows)], 0)
    normed = normalize(tokens, gain[...])
    asking = jnp.concatenate([normed[256 * n : 256 * n + 64] for n in range(windows)], 0)
    queries = dot(asking.astype(BF16), mixer[:, :384]).astype(BF16)
    pairs = dot(normed.astype(BF16), mixer[:, 384:]).astype(BF16)
    contexts = []
    for n in range(windows):
        asked = queries[64 * n : 64 * (n + 1)]
        held = pairs[256 * n : 256 * (n + 1)]
        contexts.append(
            jnp.concatenate(
                [
                    attend_group(
                        asked[:, g * 128 : (g + 1) * 128],
                        held[:, g * 128 : (g + 1) * 128],
                        held[:, 384 + g * 128 : 384 + (g + 1) * 128],
                        4,
                    )
                    for g in range(3)
                ],
                1,
            )
        )
    result = (mine + dot(jnp.concatenate(contexts, 0), output[...])).astype(BF16)
    for n in range(windows):
        out_ref[n] = result[64 * n : 64 * (n + 1)]


def coarse(tiles, *weights):
    samples = tiles[0].shape[0]
    step = 4
    spec = pl.BlockSpec((step, 64, 384), lambda n: (n, 0, 0))
    return pl.pallas_call(
        coarse_body,
        grid=(samples // step,),
        in_specs=[spec] * 4 + [whole(w) for w in weights],
        out_specs=spec,
        out_shape=jax.ShapeDtypeStruct((samples, 64, 384), BF16),
        compiler_params=pltpu.CompilerParams(vmem_limit_bytes=24 << 20),
        name="coarse",
    )(*tiles, *weights)


def shards(
    rows,
    columns,
    fields,
    gain_window,
    mixer_fine,
    output_fine,
    gain_hidden,
    expand,
    contract,
    gain_merge,
    merge_weight,
    gain_coarse,
    mixer_coarse,
    output_coarse,
):
    samples = fields.shape[0]

    def moved(value, target, back=False):
        pairs = []
        for p in range(rows):
            for q in range(columns):
                to_p, to_q = target(p, q)
                pair = (p * columns + q, (to_p % rows) * columns + to_q % columns)
                pairs.append(pair[::-1] if back else pair)
        return lax.ppermute(value, ("gx", "gy"), pairs)

    def to_row(p, q):
        return p - 1, q

    def to_col(p, q):
        return p, q - 1 if p % 2 else q + 1

    def to_diag(p, q):
        return p - 1, q + 1 if p % 2 else q - 1

    odd = (lax.axis_index("gx") % 2).astype(jnp.int32).reshape(1)
    own, col, row, diag = pack(odd, fields)
    col = moved(col, to_col)
    row = moved(row, to_row)
    diag = moved(diag, to_diag)
    mixer = jnp.pad(mixer_fine.reshape(192, 3, 192), ((0, 0), (0, 0), (0, 64))).reshape(192, 768)
    own, col, row, diag = fine(
        own,
        col,
        row,
        diag,
        gain_window.reshape(1, 192),
        mixer,
        jnp.pad(output_fine, ((0, 64), (0, 0))),
        gain_hidden.reshape(1, 192),
        expand,
        contract,
        gain_merge.reshape(4, 192),
        merge_weight.reshape(4, 192, 384),
    )
    col = moved(col, to_col, True)
    row = moved(row, to_row, True)
    diag = moved(diag, to_diag, True)
    tile = assemble(odd, own, col, row, diag)
    beside = moved(tile, lambda p, q: (p ^ 1, q))
    twin = moved(tile, lambda p, q: (p, q ^ 1))
    beyond = moved(beside, lambda p, q: (p, q ^ 1))
    result = coarse(
        (tile, beside, twin, beyond), gain_coarse.reshape(1, 384), mixer_coarse, output_coarse
    )
    shape = (samples, 8, 8, 384)
    return tile.reshape(shape), result.reshape(shape)


def solution(mesh):
    place = P(None, "gx", "gy", None)
    body = functools.partial(shards, mesh.shape["gx"], mesh.shape["gy"])
    return jax.shard_map(
        body, mesh=mesh, in_specs=(place,) + (P(),) * 11, out_specs=(place, place), check_vma=False
    )
```

```python
import functools
import math

import jax
import jax.numpy as jnp
from jax import lax
from jax.experimental import pallas as pl
from jax.experimental.pallas import tpu as pltpu
from jax.sharding import PartitionSpec as P


HEAD = 32
EPS = 1e-05
SCALE = math.log2(math.e) / math.sqrt(HEAD)
F32 = jnp.float32
BF16 = jnp.bfloat16


def dot(a, b):
    return jnp.dot(a, b, preferred_element_type=F32)


def dot_nt(a, b):
    return lax.dot_general(a, b, (((1,), (1,)), ((), ())), preferred_element_type=F32)


def iota(shape, dim):
    return lax.broadcasted_iota(jnp.int32, shape, dim)


def one_hot(rows, source):
    return jnp.where(iota((rows, rows), 1) == source, 1.0, 0.0).astype(BF16)


def normalize(values, scaling):
    center = values - jnp.mean(values, -1, keepdims=True)
    spread = jnp.mean(center * center, -1, keepdims=True)
    return center * lax.rsqrt(spread + EPS) * scaling


def pack_body(odd_ref, x_ref, own_ref, col_ref, row_ref, diag_ref, order_ref):
    @pl.when(pl.program_id(0) == 0)
    def _():
        odd = odd_ref[0]
        place = iota((256, 256), 0)
        piece = place // 64
        phase = (place // 16) % 4
        i = 2 * ((place // 4) % 4) + phase % 2
        j = 2 * (place % 4) + phase // 2
        bottom = jnp.where(piece < 2, 1, 0)
        keep = jnp.where((piece == 0) | (piece == 3), odd, 1 - odd)
        order_ref[...] = one_hot(256, (8 * bottom + i) * 16 + 8 * keep + j)

    samples = x_ref.shape[0]
    for n in range(samples):
        tokens = x_ref[n].reshape(256, 192)
        sorted_tokens = dot(order_ref[...], tokens)
        own_ref[n] = sorted_tokens[:64].astype(BF16)
        for slot, ref in enumerate((col_ref, row_ref, diag_ref)):
            part = sorted_tokens[64 * (slot + 1) : 64 * (slot + 2)]
            ref[n, :64, :] = part[:, :128].astype(BF16)
            ref[n, 64:, :] = jnp.concatenate([part[:32, 128:], part[32:, 128:]], 1).astype(BF16)


def pack(odd, fields):
    samples = fields.shape[0]
    step = 2
    piece = jax.ShapeDtypeStruct((samples, 96, 128), BF16)
    piece_spec = pl.BlockSpec((step, 96, 128), lambda n: (n, 0, 0))
    return pl.pallas_call(
        pack_body,
        grid=(samples // step,),
        in_specs=[
            pl.BlockSpec(memory_space=pltpu.SMEM),
            pl.BlockSpec((step, 16, 16, 192), lambda n: (n, 0, 0, 0)),
        ],
        out_specs=[pl.BlockSpec((step, 64, 192), lambda n: (n, 0, 0))] + [piece_spec] * 3,
        out_shape=[jax.ShapeDtypeStruct((samples, 64, 192), BF16)] + [piece] * 3,
        scratch_shapes=[pltpu.VMEM((256, 256), BF16)],
        compiler_params=pltpu.CompilerParams(vmem_limit_bytes=16 << 20),
        name="pack",
    )(odd, fields)


def unpack(ref, n):
    low = ref[n, :64, :].astype(F32)
    high = ref[n, 64:, :].astype(F32)
    turned = pltpu.roll(high, 64, 1)
    return jnp.concatenate([low, jnp.concatenate([high, turned], 0)[:, :64]], 1)


def head_mask(head, last):
    lane = iota((1, 128), 1) // HEAD
    return jnp.where(jnp.minimum(lane, last) == head, 1.0, 0.0).astype(BF16)


def attend_group(queries, keys, values, heads):
    rows = queries.shape[0]
    length = keys.shape[0]
    masks = [head_mask(head, heads - 1) for head in range(heads)]
    scores = dot_nt(jnp.concatenate([queries * mask for mask in masks], 0), keys)
    highest = jnp.max(scores, -1, keepdims=True) * SCALE
    power = jnp.exp2(scores * SCALE - highest).astype(BF16)
    parts = range(heads)
    powers = [power[head * rows : (head + 1) * rows] for head in parts]
    weights = [
        jnp.concatenate([values * mask, jnp.broadcast_to(mask, (length, 128))], 1) for mask in masks
    ]
    sums = dot(jnp.concatenate(powers, 1), jnp.concatenate(weights, 0))
    return highest, masks, sums[:, :128], sums[:, 128:]


def attend_whole(queries, keys, values, heads):
    _, _, weighted, total = attend_group(queries, keys, values, heads)
    return (weighted / total).astype(BF16)


def attend_part(queries, keys, values, heads):
    rows = queries.shape[0]
    highest, masks, weighted, total = attend_group(queries, keys, values, heads)
    top = sum(
        highest[head * rows : (head + 1) * rows] * masks[head].astype(F32) for head in range(heads)
    )
    return top, weighted, total


def gelu(x):
    return 0.5 * x * (1.0 + lax.erf(x * math.sqrt(0.5)))


def fine_body(
    own_ref,
    col_ref,
    row_ref,
    diag_ref,
    gain_window,
    mixer,
    output,
    gain_hidden,
    expand,
    contract,
    gain_merge,
    merge_weight,
    own_out,
    col_out,
    row_out,
    diag_out,
):
    windows = own_ref.shape[0]
    tokens = jnp.concatenate(
        [
            part
            for n in range(windows)
            for part in (
                own_ref[n].astype(F32),
                unpack(col_ref, n),
                unpack(row_ref, n),
                unpack(diag_ref, n),
            )
        ],
        0,
    )
    normed = normalize(tokens, gain_window[...]).astype(BF16)
    mixed = dot(normed, mixer[...]).astype(BF16)
    contexts = []
    for n in range(windows):
        one = mixed[256 * n : 256 * (n + 1)]
        contexts.append(
            jnp.concatenate(
                [
                    attend_whole(one[:, :128], one[:, 256:384], one[:, 512:640], 4),
                    attend_whole(one[:, 128:256], one[:, 384:512], one[:, 640:], 2),
                ],
                1,
            )
        )
    context = jnp.concatenate(contexts, 0)
    attended = (tokens + dot(context, output[...])).astype(BF16).astype(F32)
    normed = normalize(attended, gain_hidden[...]).astype(BF16)
    hidden = gelu(dot(normed, expand[...])).astype(BF16)
    refined = (attended + dot(hidden, contract[...])).astype(BF16).astype(F32)
    phases = [
        jnp.concatenate(
            [
                refined[64 * piece + 16 * k : 64 * piece + 16 * (k + 1)]
                for piece in range(4 * windows)
            ],
            0,
        )
        for k in range(4)
    ]
    mean = sum(jnp.sum(part, -1, keepdims=True) for part in phases) / 768.0
    centers = [part - mean for part in phases]
    spread = sum(jnp.sum(part * part, -1, keepdims=True) for part in centers) / 768.0
    ratio = lax.rsqrt(spread + EPS)
    merged = sum(
        dot((centers[k] * ratio * gain_merge[k : k + 1, :]).astype(BF16), merge_weight[k])
        for k in range(4)
    ).astype(BF16)
    for n in range(windows):
        for slot, ref in enumerate((own_out, col_out, row_out, diag_out)):
            ref[n] = merged[64 * n + 16 * slot : 64 * n + 16 * (slot + 1)]


def whole(array):
    return pl.BlockSpec(array.shape, lambda n: (0,) * array.ndim)


def fine(own, col, row, diag, *weights):
    samples = own.shape[0]
    step = 4
    piece_spec = pl.BlockSpec((step, 96, 128), lambda n: (n, 0, 0))
    return pl.pallas_call(
        fine_body,
        grid=(samples // step,),
        in_specs=[pl.BlockSpec((step, 64, 192), lambda n: (n, 0, 0))]
        + [piece_spec] * 3
        + [whole(w) for w in weights],
        out_specs=[pl.BlockSpec((step, 16, 384), lambda n: (n, 0, 0))] * 4,
        out_shape=[jax.ShapeDtypeStruct((samples, 16, 384), BF16)] * 4,
        compiler_params=pltpu.CompilerParams(vmem_limit_bytes=32 << 20),
        name="fine",
    )(own, col, row, diag, *weights)


def assemble_body(odd_ref, own_ref, col_ref, row_ref, diag_ref, out_ref):
    odd = odd_ref[0]
    place = iota((64, 64), 0)
    r = place // 8
    c = place % 8
    bottom = r // 4
    keep = jnp.where(c // 4 == odd, 1, 0)
    piece = jnp.where(bottom == 1, 1 - keep, 2 + keep)
    order = one_hot(64, piece * 16 + (r % 4) * 4 + c % 4)
    for n in range(own_ref.shape[0]):
        parts = jnp.concatenate([own_ref[n], col_ref[n], row_ref[n], diag_ref[n]], 0)
        out_ref[n] = dot(order, parts).astype(BF16)


def assemble(odd, *pieces):
    samples = pieces[0].shape[0]
    vmem = pl.BlockSpec(memory_space=pltpu.VMEM)
    return pl.pallas_call(
        assemble_body,
        in_specs=[pl.BlockSpec(memory_space=pltpu.SMEM)] + [vmem] * 4,
        out_specs=vmem,
        out_shape=jax.ShapeDtypeStruct((samples, 64, 384), BF16),
        compiler_params=pltpu.CompilerParams(vmem_limit_bytes=8 << 20),
        name="assemble",
    )(odd, *pieces)


def group(values, n, rows, g):
    return values[rows * n : rows * (n + 1), 128 * g : 128 * (g + 1)]


def coarse_first_body(mine_ref, twin_ref, gain, mixer, query_ref, top_ref, sum_ref, total_ref):
    windows = mine_ref.shape[0]
    tokens = jnp.concatenate(
        [ref[n].astype(F32) for ref in (mine_ref, twin_ref) for n in range(windows)], 0
    )
    normed = normalize(tokens, gain[...]).astype(BF16)
    queries = dot(normed[: 64 * windows], mixer[:, :384]).astype(BF16)
    pairs = dot(normed, mixer[:, 384:]).astype(BF16)
    for n in range(windows):
        query_ref[n] = queries[64 * n : 64 * (n + 1)]
        held = jnp.concatenate(
            [pairs[64 * k : 64 * (k + 1)] for k in (n, n + windows)], 0
        )
        for g in range(3):
            lanes = slice(128 * g, 128 * (g + 1))
            top, weighted, total = attend_part(
                group(queries, n, 64, g), group(held, 0, 128, g), group(held, 0, 128, g + 3), 4
            )
            top_ref[n, :, lanes] = top
            sum_ref[n, :, lanes] = weighted
            total_ref[n, :, lanes] = total


def coarse_second_body(
    mine_ref, a_ref, b_ref, query_ref, top_ref, sum_ref, total_ref, gain, mixer, output, out_ref
):
    windows = mine_ref.shape[0]
    tokens = jnp.concatenate(
        [ref[n].astype(F32) for n in range(windows) for ref in (a_ref, b_ref)], 0
    )
    normed = normalize(tokens, gain[...]).astype(BF16)
    pairs = dot(normed, mixer[:, 384:]).astype(BF16)
    contexts = []
    for n in range(windows):
        parts = []
        for g in range(3):
            lanes = slice(128 * g, 128 * (g + 1))
            top, weighted, total = attend_part(
                query_ref[n, :, lanes], group(pairs, n, 128, g), group(pairs, n, 128, g + 3), 4
            )
            before = top_ref[n, :, lanes]
            highest = jnp.maximum(before, top)
            old = jnp.exp2(before - highest)
            new = jnp.exp2(top - highest)
            weighted = sum_ref[n, :, lanes] * old + weighted * new
            total = total_ref[n, :, lanes] * old + total * new
            parts.append((weighted / total).astype(BF16))
        contexts.append(jnp.concatenate(parts, 1))
    update = dot(jnp.concatenate(contexts, 0), output[...])
    for n in range(windows):
        mine = mine_ref[n].astype(F32)
        out_ref[n] = (mine + update[64 * n : 64 * (n + 1)]).astype(BF16)


def coarse_call(body, step, tiles, weights, kinds):
    samples = tiles[0].shape[0]
    spec = pl.BlockSpec((step, 64, 384), lambda n: (n, 0, 0))
    shapes = [jax.ShapeDtypeStruct((samples, 64, 384), kind) for kind in kinds]
    return pl.pallas_call(
        body,
        grid=(samples // step,),
        in_specs=[spec] * len(tiles) + [whole(w) for w in weights],
        out_specs=[spec] * len(kinds),
        out_shape=shapes,
        compiler_params=pltpu.CompilerParams(vmem_limit_bytes=24 << 20),
        cost_estimate=pl.CostEstimate(
            flops=2_000_000_000, transcendentals=1_000_000, bytes_accessed=4_000_000
        ),
    )(*tiles, *weights)


def shards(
    rows,
    columns,
    fields,
    gain_window,
    mixer_fine,
    output_fine,
    gain_hidden,
    expand,
    contract,
    gain_merge,
    merge_weight,
    gain_coarse,
    mixer_coarse,
    output_coarse,
):
    samples = fields.shape[0]

    def moved(value, target, back=False):
        pairs = []
        for p in range(rows):
            for q in range(columns):
                to_p, to_q = target(p, q)
                pair = (p * columns + q, (to_p % rows) * columns + to_q % columns)
                pairs.append(pair[::-1] if back else pair)
        return lax.ppermute(value, ("gx", "gy"), pairs)

    def to_row(p, q):
        return p - 1, q

    def to_col(p, q):
        return p, q - 1 if p % 2 else q + 1

    def to_diag(p, q):
        return p - 1, q + 1 if p % 2 else q - 1

    odd = (lax.axis_index("gx") % 2).astype(jnp.int32).reshape(1)
    own, col, row, diag = pack(odd, fields)
    row = moved(row, to_row)
    diag = moved(diag, to_diag)
    col = moved(col, to_col)
    mixer = jnp.pad(mixer_fine.reshape(192, 3, 192), ((0, 0), (0, 0), (0, 64))).reshape(192, 768)
    own, col, row, diag = fine(
        own,
        col,
        row,
        diag,
        gain_window.reshape(1, 192),
        mixer,
        jnp.pad(output_fine, ((0, 64), (0, 0))),
        gain_hidden.reshape(1, 192),
        expand,
        contract,
        gain_merge.reshape(4, 192),
        merge_weight.reshape(4, 192, 384),
    )
    row = moved(row, to_row, True)
    diag = moved(diag, to_diag, True)
    col = moved(col, to_col, True)
    tile = assemble(odd, own, col, row, diag)
    beside = moved(tile, lambda p, q: (p ^ 1, q))
    twin = moved(tile, lambda p, q: (p, q ^ 1))
    gain = gain_coarse.reshape(1, 384)
    first = coarse_call(
        coarse_first_body, 4, (tile, twin), (gain, mixer_coarse), (BF16, F32, F32, F32)
    )
    beyond = moved(beside, lambda p, q: (p, q ^ 1))
    (result,) = coarse_call(
        coarse_second_body,
        4,
        (tile, beside, beyond, *first),
        (gain, mixer_coarse, output_coarse),
        (BF16,),
    )
    shape = (samples, 8, 8, 384)
    return tile.reshape(shape), result.reshape(shape)


def solution(mesh):
    place = P(None, "gx", "gy", None)
    body = functools.partial(shards, mesh.shape["gx"], mesh.shape["gy"])
    return jax.shard_map(
        body, mesh=mesh, in_specs=(place,) + (P(),) * 11, out_specs=(place, place), check_vma=False
    )
```

```python
import functools
import math

import jax
import jax.numpy as jnp
from jax import lax
from jax.experimental import pallas as pl
from jax.experimental.pallas import tpu as pltpu
from jax.sharding import PartitionSpec as P


HEAD = 32
EPS = 1e-05
SCALE = math.log2(math.e) / math.sqrt(HEAD)
F32 = jnp.float32
BF16 = jnp.bfloat16


def dot(a, b):
    return jnp.dot(a, b, preferred_element_type=F32)


def dot_nt(a, b):
    return lax.dot_general(a, b, (((1,), (1,)), ((), ())), preferred_element_type=F32)


def iota(shape, dim):
    return lax.broadcasted_iota(jnp.int32, shape, dim)


def one_hot(rows, source):
    return jnp.where(iota((rows, rows), 1) == source, 1.0, 0.0).astype(BF16)


def normalize(values, scaling):
    center = values - jnp.mean(values, -1, keepdims=True)
    spread = jnp.mean(center * center, -1, keepdims=True)
    return center * lax.rsqrt(spread + EPS) * scaling


def pack_body(odd_ref, x_ref, own_ref, col_ref, row_ref, diag_ref, order_ref):
    @pl.when(pl.program_id(0) == 0)
    def _():
        odd = odd_ref[0]
        place = iota((256, 256), 0)
        piece = place // 64
        phase = (place // 16) % 4
        i = 2 * ((place // 4) % 4) + phase % 2
        j = 2 * (place % 4) + phase // 2
        bottom = jnp.where(piece < 2, 1, 0)
        keep = jnp.where((piece == 0) | (piece == 3), odd, 1 - odd)
        order_ref[...] = one_hot(256, (8 * bottom + i) * 16 + 8 * keep + j)

    samples = x_ref.shape[0]
    for n in range(samples):
        tokens = x_ref[n].reshape(256, 192)
        sorted_tokens = dot(order_ref[...], tokens)
        own_ref[n] = sorted_tokens[:64].astype(BF16)
        for slot, ref in enumerate((col_ref, row_ref, diag_ref)):
            part = sorted_tokens[64 * (slot + 1) : 64 * (slot + 2)]
            ref[n, :64, :] = part[:, :128].astype(BF16)
            ref[n, 64:, :] = jnp.concatenate([part[:32, 128:], part[32:, 128:]], 1).astype(BF16)


def pack(odd, fields):
    samples = fields.shape[0]
    step = 2
    piece = jax.ShapeDtypeStruct((samples, 96, 128), BF16)
    piece_spec = pl.BlockSpec((step, 96, 128), lambda n: (n, 0, 0))
    return pl.pallas_call(
        pack_body,
        grid=(samples // step,),
        in_specs=[
            pl.BlockSpec(memory_space=pltpu.SMEM),
            pl.BlockSpec((step, 16, 16, 192), lambda n: (n, 0, 0, 0)),
        ],
        out_specs=[pl.BlockSpec((step, 64, 192), lambda n: (n, 0, 0))] + [piece_spec] * 3,
        out_shape=[jax.ShapeDtypeStruct((samples, 64, 192), BF16)] + [piece] * 3,
        scratch_shapes=[pltpu.VMEM((256, 256), BF16)],
        compiler_params=pltpu.CompilerParams(vmem_limit_bytes=16 << 20),
        name="pack",
    )(odd, fields)


def unpack(ref, n):
    low = ref[n, :64, :].astype(F32)
    high = ref[n, 64:, :].astype(F32)
    turned = pltpu.roll(high, 64, 1)
    return jnp.concatenate([low, jnp.concatenate([high, turned], 0)[:, :64]], 1)


def head_mask(head, last):
    lane = iota((1, 128), 1) // HEAD
    return jnp.where(jnp.minimum(lane, last) == head, 1.0, 0.0).astype(BF16)


def attend_group(queries, keys, values, heads):
    rows = queries.shape[0]
    length = keys.shape[0]
    masks = [head_mask(head, heads - 1) for head in range(heads)]
    scores = dot_nt(jnp.concatenate([queries * mask for mask in masks], 0), keys)
    highest = jnp.max(scores, -1, keepdims=True) * SCALE
    power = jnp.exp2(scores * SCALE - highest).astype(BF16)
    parts = range(heads)
    powers = [power[head * rows : (head + 1) * rows] for head in parts]
    weights = [
        jnp.concatenate([values * mask, jnp.broadcast_to(mask, (length, 128))], 1) for mask in masks
    ]
    sums = dot(jnp.concatenate(powers, 1), jnp.concatenate(weights, 0))
    return highest, masks, sums[:, :128], sums[:, 128:]


def attend_whole(queries, keys, values, heads):
    _, _, weighted, total = attend_group(queries, keys, values, heads)
    return (weighted / total).astype(BF16)


def attend_part(queries, keys, values, heads):
    rows = queries.shape[0]
    highest, masks, weighted, total = attend_group(queries, keys, values, heads)
    top = sum(
        highest[head * rows : (head + 1) * rows] * masks[head].astype(F32) for head in range(heads)
    )
    return top, weighted, total


def gelu(x):
    return 0.5 * x * (1.0 + lax.erf(x * math.sqrt(0.5)))


def fine_body(
    own_ref,
    col_ref,
    row_ref,
    diag_ref,
    gains,
    mixer,
    output,
    expand,
    contract,
    merge_weight,
    own_out,
    col_out,
    row_out,
    diag_out,
):
    windows = own_ref.shape[0]
    tokens = jnp.concatenate(
        [
            part
            for n in range(windows)
            for part in (
                own_ref[n].astype(F32),
                unpack(col_ref, n),
                unpack(row_ref, n),
                unpack(diag_ref, n),
            )
        ],
        0,
    )
    normed = normalize(tokens, gains[0:1, :]).astype(BF16)
    mixed = dot(normed, mixer[...]).astype(BF16)
    contexts = []
    for n in range(windows):
        one = mixed[256 * n : 256 * (n + 1)]
        contexts.append(
            jnp.concatenate(
                [
                    attend_whole(one[:, :128], one[:, 256:384], one[:, 512:640], 4),
                    attend_whole(one[:, 128:256], one[:, 384:512], one[:, 640:], 2),
                ],
                1,
            )
        )
    context = jnp.concatenate(contexts, 0)
    attended = (tokens + dot(context, output[...])).astype(BF16).astype(F32)
    normed = normalize(attended, gains[1:2, :]).astype(BF16)
    hidden = gelu(dot(normed, expand[...])).astype(BF16)
    refined = (attended + dot(hidden, contract[...])).astype(BF16).astype(F32)
    phases = [
        jnp.concatenate(
            [
                refined[64 * piece + 16 * k : 64 * piece + 16 * (k + 1)]
                for piece in range(4 * windows)
            ],
            0,
        )
        for k in range(4)
    ]
    mean = sum(jnp.sum(part, -1, keepdims=True) for part in phases) / 768.0
    centers = [part - mean for part in phases]
    spread = sum(jnp.sum(part * part, -1, keepdims=True) for part in centers) / 768.0
    ratio = lax.rsqrt(spread + EPS)
    merged = sum(
        dot((centers[k] * ratio * gains[k + 2 : k + 3, :]).astype(BF16), merge_weight[k])
        for k in range(4)
    ).astype(BF16)
    for n in range(windows):
        for slot, ref in enumerate((own_out, col_out, row_out, diag_out)):
            ref[n] = merged[64 * n + 16 * slot : 64 * n + 16 * (slot + 1)]


def whole(array):
    return pl.BlockSpec(array.shape, lambda n: (0,) * array.ndim)


def fine(own, col, row, diag, *weights):
    samples = own.shape[0]
    step = 4
    piece_spec = pl.BlockSpec((step, 96, 128), lambda n: (n, 0, 0))
    return pl.pallas_call(
        fine_body,
        grid=(samples // step,),
        in_specs=[pl.BlockSpec((step, 64, 192), lambda n: (n, 0, 0))]
        + [piece_spec] * 3
        + [whole(w) for w in weights],
        out_specs=[pl.BlockSpec((step, 16, 384), lambda n: (n, 0, 0))] * 4,
        out_shape=[jax.ShapeDtypeStruct((samples, 16, 384), BF16)] * 4,
        compiler_params=pltpu.CompilerParams(vmem_limit_bytes=32 << 20),
        name="fine",
    )(own, col, row, diag, *weights)


def assemble_body(odd_ref, own_ref, col_ref, row_ref, diag_ref, out_ref):
    odd = odd_ref[0]
    place = iota((64, 64), 0)
    r = place // 8
    c = place % 8
    bottom = r // 4
    keep = jnp.where(c // 4 == odd, 1, 0)
    piece = jnp.where(bottom == 1, 1 - keep, 2 + keep)
    order = one_hot(64, piece * 16 + (r % 4) * 4 + c % 4)
    for n in range(own_ref.shape[0]):
        parts = jnp.concatenate([own_ref[n], col_ref[n], row_ref[n], diag_ref[n]], 0)
        out_ref[n] = dot(order, parts).astype(BF16)


def assemble(odd, *pieces):
    samples = pieces[0].shape[0]
    vmem = pl.BlockSpec(memory_space=pltpu.VMEM)
    return pl.pallas_call(
        assemble_body,
        in_specs=[pl.BlockSpec(memory_space=pltpu.SMEM)] + [vmem] * 4,
        out_specs=vmem,
        out_shape=pltpu.VMEM((samples, 64, 384), BF16),
        compiler_params=pltpu.CompilerParams(vmem_limit_bytes=8 << 20),
        name="assemble",
    )(odd, *pieces)


def group(values, n, rows, g):
    return values[rows * n : rows * (n + 1), 128 * g : 128 * (g + 1)]


def coarse_first_body(mine_ref, twin_ref, gain, mixer, query_ref, top_ref, sum_ref, total_ref):
    windows = mine_ref.shape[0]
    tokens = jnp.concatenate(
        [ref[n].astype(F32) for ref in (mine_ref, twin_ref) for n in range(windows)], 0
    )
    normed = normalize(tokens, gain[...]).astype(BF16)
    queries = dot(normed[: 64 * windows], mixer[:, :384]).astype(BF16)
    pairs = dot(normed, mixer[:, 384:]).astype(BF16)
    for n in range(windows):
        query_ref[n] = queries[64 * n : 64 * (n + 1)]
        held = jnp.concatenate(
            [pairs[64 * k : 64 * (k + 1)] for k in (n, n + windows)], 0
        )
        for g in range(3):
            lanes = slice(128 * g, 128 * (g + 1))
            top, weighted, total = attend_part(
                group(queries, n, 64, g), group(held, 0, 128, g), group(held, 0, 128, g + 3), 4
            )
            top_ref[n, :, lanes] = top
            sum_ref[n, :, lanes] = weighted
            total_ref[n, :, lanes] = total


def coarse_second_body(
    mine_ref, a_ref, b_ref, query_ref, top_ref, sum_ref, total_ref, gain, mixer, output, out_ref
):
    windows = mine_ref.shape[0]
    tokens = jnp.concatenate(
        [ref[n].astype(F32) for n in range(windows) for ref in (a_ref, b_ref)], 0
    )
    normed = normalize(tokens, gain[...]).astype(BF16)
    pairs = dot(normed, mixer[:, 384:]).astype(BF16)
    contexts = []
    for n in range(windows):
        parts = []
        for g in range(3):
            lanes = slice(128 * g, 128 * (g + 1))
            top, weighted, total = attend_part(
                query_ref[n, :, lanes], group(pairs, n, 128, g), group(pairs, n, 128, g + 3), 4
            )
            before = top_ref[n, :, lanes]
            highest = jnp.maximum(before, top)
            old = jnp.exp2(before - highest)
            new = jnp.exp2(top - highest)
            weighted = sum_ref[n, :, lanes] * old + weighted * new
            total = total_ref[n, :, lanes] * old + total * new
            parts.append((weighted / total).astype(BF16))
        contexts.append(jnp.concatenate(parts, 1))
    update = dot(jnp.concatenate(contexts, 0), output[...])
    for n in range(windows):
        mine = mine_ref[n].astype(F32)
        out_ref[n] = (mine + update[64 * n : 64 * (n + 1)]).astype(BF16)


def coarse_call(body, step, tiles, weights, kinds):
    samples = tiles[0].shape[0]
    spec = pl.BlockSpec((step, 64, 384), lambda n: (n, 0, 0))
    shapes = [jax.ShapeDtypeStruct((samples, 64, 384), kind) for kind in kinds]
    return pl.pallas_call(
        body,
        grid=(samples // step,),
        in_specs=[spec] * len(tiles) + [whole(w) for w in weights],
        out_specs=[spec] * len(kinds),
        out_shape=shapes,
        compiler_params=pltpu.CompilerParams(vmem_limit_bytes=24 << 20),
        cost_estimate=pl.CostEstimate(
            flops=2_000_000_000, transcendentals=1_000_000, bytes_accessed=4_000_000
        ),
    )(*tiles, *weights)


def shards(
    rows,
    columns,
    fields,
    gain_window,
    mixer_fine,
    output_fine,
    gain_hidden,
    expand,
    contract,
    gain_merge,
    merge_weight,
    gain_coarse,
    mixer_coarse,
    output_coarse,
):
    samples = fields.shape[0]

    def moved(value, target, back=False):
        pairs = []
        for p in range(rows):
            for q in range(columns):
                to_p, to_q = target(p, q)
                pair = (p * columns + q, (to_p % rows) * columns + to_q % columns)
                pairs.append(pair[::-1] if back else pair)
        return lax.ppermute(value, ("gx", "gy"), pairs)

    def to_row(p, q):
        return p - 1, q

    def to_col(p, q):
        return p, q - 1 if p % 2 else q + 1

    def to_diag(p, q):
        return p - 1, q + 1 if p % 2 else q - 1

    odd = (lax.axis_index("gx") % 2).astype(jnp.int32).reshape(1)
    own, col, row, diag = pack(odd, fields)
    row = moved(row, to_row)
    diag = moved(diag, to_diag)
    col = moved(col, to_col)
    gains = jnp.concatenate([gain_window, gain_hidden, gain_merge]).reshape(6, 192)
    mixer = jnp.pad(mixer_fine.reshape(192, 3, 192), ((0, 0), (0, 0), (0, 64))).reshape(192, 768)
    own, col, row, diag = fine(
        own,
        col,
        row,
        diag,
        gains,
        mixer,
        jnp.pad(output_fine, ((0, 64), (0, 0))),
        expand,
        contract,
        merge_weight.reshape(4, 192, 384),
    )
    row = moved(row, to_row, True)
    diag = moved(diag, to_diag, True)
    col = moved(col, to_col, True)
    tile = assemble(odd, own, col, row, diag)
    beside = moved(tile, lambda p, q: (p ^ 1, q))
    twin = moved(tile, lambda p, q: (p, q ^ 1))
    gain = gain_coarse.reshape(1, 384)
    first = coarse_call(
        coarse_first_body, 4, (tile, twin), (gain, mixer_coarse), (BF16, F32, F32, F32)
    )
    beyond = moved(beside, lambda p, q: (p, q ^ 1))
    (result,) = coarse_call(
        coarse_second_body,
        4,
        (tile, beside, beyond, *first),
        (gain, mixer_coarse, output_coarse),
        (BF16,),
    )
    shape = (samples, 8, 8, 384)
    return tile.reshape(shape), result.reshape(shape)


def solution(mesh):
    place = P(None, "gx", "gy", None)
    body = functools.partial(shards, mesh.shape["gx"], mesh.shape["gy"])
    return jax.shard_map(
        body, mesh=mesh, in_specs=(place,) + (P(),) * 11, out_specs=(place, place), check_vma=False
    )
```

```python
import functools
import math

import jax
import jax.numpy as jnp
from jax import lax
from jax.experimental import pallas as pl
from jax.experimental.pallas import tpu as pltpu
from jax.sharding import PartitionSpec as P


HEAD = 32
EPS = 1e-05
SCALE = math.log2(math.e) / math.sqrt(HEAD)
F32 = jnp.float32
BF16 = jnp.bfloat16


def dot(a, b):
    return jnp.dot(a, b, preferred_element_type=F32)


def dot_nt(a, b):
    return lax.dot_general(a, b, (((1,), (1,)), ((), ())), preferred_element_type=F32)


def iota(shape, dim):
    return lax.broadcasted_iota(jnp.int32, shape, dim)


def one_hot(rows, source):
    return jnp.where(iota((rows, rows), 1) == source, 1.0, 0.0).astype(BF16)


def normalize(values, scaling):
    center = values - jnp.mean(values, -1, keepdims=True)
    spread = jnp.mean(center * center, -1, keepdims=True)
    return center * lax.rsqrt(spread + EPS) * scaling


def pack_body(odd_ref, x_ref, own_ref, col_ref, row_ref, diag_ref, order_ref):
    @pl.when(pl.program_id(0) == 0)
    def _():
        odd = odd_ref[0]
        place = iota((256, 256), 0)
        piece = place // 64
        phase = (place // 16) % 4
        i = 2 * ((place // 4) % 4) + phase % 2
        j = 2 * (place % 4) + phase // 2
        bottom = jnp.where(piece < 2, 1, 0)
        keep = jnp.where((piece == 0) | (piece == 3), odd, 1 - odd)
        order_ref[...] = one_hot(256, (8 * bottom + i) * 16 + 8 * keep + j)

    samples = x_ref.shape[0]
    for n in range(samples):
        tokens = x_ref[n].reshape(256, 192)
        sorted_tokens = dot(order_ref[...], tokens)
        own_ref[n] = sorted_tokens[:64].astype(BF16)
        for slot, ref in enumerate((col_ref, row_ref, diag_ref)):
            part = sorted_tokens[64 * (slot + 1) : 64 * (slot + 2)]
            ref[n, :64, :] = part[:, :128].astype(BF16)
            ref[n, 64:, :] = jnp.concatenate([part[:32, 128:], part[32:, 128:]], 1).astype(BF16)


def pack(odd, fields):
    samples = fields.shape[0]
    step = samples
    piece = jax.ShapeDtypeStruct((samples, 96, 128), BF16)
    piece_spec = pl.BlockSpec((step, 96, 128), lambda n: (n, 0, 0))
    return pl.pallas_call(
        pack_body,
        grid=(samples // step,),
        in_specs=[
            pl.BlockSpec(memory_space=pltpu.SMEM),
            pl.BlockSpec((step, 16, 16, 192), lambda n: (n, 0, 0, 0)),
        ],
        out_specs=[pl.BlockSpec((step, 64, 192), lambda n: (n, 0, 0))] + [piece_spec] * 3,
        out_shape=[jax.ShapeDtypeStruct((samples, 64, 192), BF16)] + [piece] * 3,
        scratch_shapes=[pltpu.VMEM((256, 256), BF16)],
        compiler_params=pltpu.CompilerParams(vmem_limit_bytes=16 << 20),
        name="pack",
    )(odd, fields)


def unpack(ref, n):
    low = ref[n, :64, :].astype(F32)
    high = ref[n, 64:, :].astype(F32)
    turned = pltpu.roll(high, 64, 1)
    return jnp.concatenate([low, jnp.concatenate([high, turned], 0)[:, :64]], 1)


def head_mask(head, last):
    lane = iota((1, 128), 1) // HEAD
    return jnp.where(jnp.minimum(lane, last) == head, 1.0, 0.0).astype(BF16)


def score(queries, keys, heads):
    masks = [head_mask(head, heads - 1) for head in range(heads)]
    scores = dot_nt(jnp.concatenate([queries * mask for mask in masks], 0), keys)
    highest = jnp.max(scores, -1, keepdims=True) * SCALE
    return highest, jnp.exp2(scores * SCALE - highest).astype(BF16), masks


def attend_whole(queries, keys, values, heads):
    rows = queries.shape[0]
    length = keys.shape[0]
    _, power, masks = score(queries, keys, heads)
    powers = [power[head * rows : (head + 1) * rows] for head in range(heads)]
    weights = [
        jnp.concatenate([values * mask, jnp.broadcast_to(mask, (length, 128))], 1) for mask in masks
    ]
    sums = dot(jnp.concatenate(powers, 1), jnp.concatenate(weights, 0))
    return (sums[:, :128] / sums[:, 128:]).astype(BF16)


def attend_part(queries, keys, values, heads):
    rows = queries.shape[0]
    highest, power, _ = score(queries, keys, heads)
    sums = dot(power, jnp.concatenate([values, jnp.ones(values.shape, BF16)], 1))
    lane = iota((1, 128), 1) // HEAD

    def spread(stacked):
        parts = [stacked[head * rows : (head + 1) * rows] for head in range(heads)]
        result = jnp.broadcast_to(parts[-1], (rows, 128))
        for head in reversed(range(heads - 1)):
            result = jnp.where(lane <= head, parts[head], result)
        return result

    return spread(highest), spread(sums[:, :128]), spread(sums[:, 128:])


def gelu(x):
    return 0.5 * x * (1.0 + lax.erf(x * math.sqrt(0.5)))


def fine_body(
    own_ref,
    col_ref,
    row_ref,
    diag_ref,
    gains,
    mixer,
    output,
    expand,
    contract,
    merge_weight,
    own_out,
    col_out,
    row_out,
    diag_out,
):
    windows = own_ref.shape[0]
    tokens = jnp.concatenate(
        [
            part
            for n in range(windows)
            for part in (
                own_ref[n].astype(F32),
                unpack(col_ref, n),
                unpack(row_ref, n),
                unpack(diag_ref, n),
            )
        ],
        0,
    )
    normed = normalize(tokens, gains[0:1, :]).astype(BF16)
    mixed = dot(normed, mixer[...]).astype(BF16)
    contexts = []
    for n in range(windows):
        one = mixed[256 * n : 256 * (n + 1)]
        contexts.append(
            jnp.concatenate(
                [
                    attend_whole(one[:, :128], one[:, 256:384], one[:, 512:640], 4),
                    attend_whole(one[:, 128:256], one[:, 384:512], one[:, 640:], 2),
                ],
                1,
            )
        )
    context = jnp.concatenate(contexts, 0)
    attended = (tokens + dot(context, output[...])).astype(BF16).astype(F32)
    normed = normalize(attended, gains[1:2, :]).astype(BF16)
    hidden = gelu(dot(normed, expand[...])).astype(BF16)
    refined = (attended + dot(hidden, contract[...])).astype(BF16).astype(F32)
    phases = [
        jnp.concatenate(
            [
                refined[64 * piece + 16 * k : 64 * piece + 16 * (k + 1)]
                for piece in range(4 * windows)
            ],
            0,
        )
        for k in range(4)
    ]
    mean = sum(jnp.sum(part, -1, keepdims=True) for part in phases) / 768.0
    centers = [part - mean for part in phases]
    spread = sum(jnp.sum(part * part, -1, keepdims=True) for part in centers) / 768.0
    ratio = lax.rsqrt(spread + EPS)
    merged = sum(
        dot((centers[k] * ratio * gains[k + 2 : k + 3, :]).astype(BF16), merge_weight[k])
        for k in range(4)
    ).astype(BF16)
    for n in range(windows):
        for slot, ref in enumerate((own_out, col_out, row_out, diag_out)):
            ref[n] = merged[64 * n + 16 * slot : 64 * n + 16 * (slot + 1)]


def whole(array):
    return pl.BlockSpec(array.shape, lambda n: (0,) * array.ndim)


def fine(own, col, row, diag, *weights):
    samples = own.shape[0]
    step = 4
    piece_spec = pl.BlockSpec((step, 96, 128), lambda n: (n, 0, 0))
    return pl.pallas_call(
        fine_body,
        grid=(samples // step,),
        in_specs=[pl.BlockSpec((step, 64, 192), lambda n: (n, 0, 0))]
        + [piece_spec] * 3
        + [whole(w) for w in weights],
        out_specs=[pl.BlockSpec((step, 16, 384), lambda n: (n, 0, 0))] * 4,
        out_shape=[jax.ShapeDtypeStruct((samples, 16, 384), BF16)] * 4,
        compiler_params=pltpu.CompilerParams(vmem_limit_bytes=32 << 20),
        name="fine",
    )(own, col, row, diag, *weights)


def assemble_body(odd_ref, own_ref, col_ref, row_ref, diag_ref, out_ref):
    odd = odd_ref[0]
    place = iota((64, 64), 0)
    r = place // 8
    c = place % 8
    bottom = r // 4
    keep = jnp.where(c // 4 == odd, 1, 0)
    piece = jnp.where(bottom == 1, 1 - keep, 2 + keep)
    order = one_hot(64, piece * 16 + (r % 4) * 4 + c % 4)
    for n in range(own_ref.shape[0]):
        parts = jnp.concatenate([own_ref[n], col_ref[n], row_ref[n], diag_ref[n]], 0)
        out_ref[n] = dot(order, parts).astype(BF16)


def assemble(odd, *pieces):
    samples = pieces[0].shape[0]
    vmem = pl.BlockSpec(memory_space=pltpu.VMEM)
    return pl.pallas_call(
        assemble_body,
        in_specs=[pl.BlockSpec(memory_space=pltpu.SMEM)] + [vmem] * 4,
        out_specs=vmem,
        out_shape=pltpu.VMEM((samples, 64, 384), BF16),
        compiler_params=pltpu.CompilerParams(vmem_limit_bytes=8 << 20),
        name="assemble",
    )(odd, *pieces)


def group(values, n, rows, g):
    return values[rows * n : rows * (n + 1), 128 * g : 128 * (g + 1)]


def coarse_first_body(mine_ref, twin_ref, gain, mixer, query_ref, top_ref, sum_ref, total_ref):
    windows = mine_ref.shape[0]
    tokens = jnp.concatenate(
        [ref[n].astype(F32) for ref in (mine_ref, twin_ref) for n in range(windows)], 0
    )
    normed = normalize(tokens, gain[...]).astype(BF16)
    queries = dot(normed[: 64 * windows], mixer[:, :384]).astype(BF16)
    pairs = dot(normed, mixer[:, 384:]).astype(BF16)
    for n in range(windows):
        query_ref[n] = queries[64 * n : 64 * (n + 1)]
        held = jnp.concatenate(
            [pairs[64 * k : 64 * (k + 1)] for k in (n, n + windows)], 0
        )
        for g in range(3):
            lanes = slice(128 * g, 128 * (g + 1))
            top, weighted, total = attend_part(
                group(queries, n, 64, g), group(held, 0, 128, g), group(held, 0, 128, g + 3), 4
            )
            top_ref[n, :, lanes] = top
            sum_ref[n, :, lanes] = weighted
            total_ref[n, :, lanes] = total


def coarse_second_body(
    mine_ref, a_ref, b_ref, query_ref, top_ref, sum_ref, total_ref, gain, mixer, output, out_ref
):
    windows = mine_ref.shape[0]
    tokens = jnp.concatenate(
        [ref[n].astype(F32) for n in range(windows) for ref in (a_ref, b_ref)], 0
    )
    normed = normalize(tokens, gain[...]).astype(BF16)
    pairs = dot(normed, mixer[:, 384:]).astype(BF16)
    contexts = []
    for n in range(windows):
        parts = []
        for g in range(3):
            lanes = slice(128 * g, 128 * (g + 1))
            top, weighted, total = attend_part(
                query_ref[n, :, lanes], group(pairs, n, 128, g), group(pairs, n, 128, g + 3), 4
            )
            before = top_ref[n, :, lanes]
            highest = jnp.maximum(before, top)
            old = jnp.exp2(before - highest)
            new = jnp.exp2(top - highest)
            weighted = sum_ref[n, :, lanes] * old + weighted * new
            total = total_ref[n, :, lanes] * old + total * new
            parts.append((weighted / total).astype(BF16))
        contexts.append(jnp.concatenate(parts, 1))
    update = dot(jnp.concatenate(contexts, 0), output[...])
    for n in range(windows):
        mine = mine_ref[n].astype(F32)
        out_ref[n] = (mine + update[64 * n : 64 * (n + 1)]).astype(BF16)


def coarse_call(body, step, tiles, weights, kinds):
    samples = tiles[0].shape[0]
    spec = pl.BlockSpec((step, 64, 384), lambda n: (n, 0, 0))
    shapes = [jax.ShapeDtypeStruct((samples, 64, 384), kind) for kind in kinds]
    return pl.pallas_call(
        body,
        grid=(samples // step,),
        in_specs=[spec] * len(tiles) + [whole(w) for w in weights],
        out_specs=[spec] * len(kinds),
        out_shape=shapes,
        compiler_params=pltpu.CompilerParams(vmem_limit_bytes=24 << 20),
        cost_estimate=pl.CostEstimate(
            flops=2_000_000_000, transcendentals=1_000_000, bytes_accessed=4_000_000
        ),
    )(*tiles, *weights)


def shards(
    rows,
    columns,
    fields,
    gain_window,
    mixer_fine,
    output_fine,
    gain_hidden,
    expand,
    contract,
    gain_merge,
    merge_weight,
    gain_coarse,
    mixer_coarse,
    output_coarse,
):
    samples = fields.shape[0]

    def moved(value, target, back=False):
        pairs = []
        for p in range(rows):
            for q in range(columns):
                to_p, to_q = target(p, q)
                pair = (p * columns + q, (to_p % rows) * columns + to_q % columns)
                pairs.append(pair[::-1] if back else pair)
        return lax.ppermute(value, ("gx", "gy"), pairs)

    def to_row(p, q):
        return p - 1, q

    def to_col(p, q):
        return p, q - 1 if p % 2 else q + 1

    def to_diag(p, q):
        return p - 1, q + 1 if p % 2 else q - 1

    odd = (lax.axis_index("gx") % 2).astype(jnp.int32).reshape(1)
    own, col, row, diag = pack(odd, fields)
    row = moved(row, to_row)
    diag = moved(diag, to_diag)
    col = moved(col, to_col)
    gains = jnp.concatenate([gain_window, gain_hidden, gain_merge]).reshape(6, 192)
    mixer = jnp.pad(mixer_fine.reshape(192, 3, 192), ((0, 0), (0, 0), (0, 64))).reshape(192, 768)
    own, col, row, diag = fine(
        own,
        col,
        row,
        diag,
        gains,
        mixer,
        jnp.pad(output_fine, ((0, 64), (0, 0))),
        expand,
        contract,
        merge_weight.reshape(4, 192, 384),
    )
    row = moved(row, to_row, True)
    diag = moved(diag, to_diag, True)
    col = moved(col, to_col, True)
    tile = assemble(odd, own, col, row, diag)
    beside = moved(tile, lambda p, q: (p ^ 1, q))
    twin = moved(tile, lambda p, q: (p, q ^ 1))
    gain = gain_coarse.reshape(1, 384)
    first = coarse_call(
        coarse_first_body, 4, (tile, twin), (gain, mixer_coarse), (BF16, F32, F32, F32)
    )
    beyond = moved(beside, lambda p, q: (p, q ^ 1))
    (result,) = coarse_call(
        coarse_second_body,
        4,
        (tile, beside, beyond, *first),
        (gain, mixer_coarse, output_coarse),
        (BF16,),
    )
    shape = (samples, 8, 8, 384)
    return tile.reshape(shape), result.reshape(shape)


def solution(mesh):
    place = P(None, "gx", "gy", None)
    body = functools.partial(shards, mesh.shape["gx"], mesh.shape["gy"])
    return jax.shard_map(
        body, mesh=mesh, in_specs=(place,) + (P(),) * 11, out_specs=(place, place), check_vma=False
    )
```
